256 devices in a mesh: freq: 32 (over y, z), pts: 8 (over x, core).
Axes of the slice: x: 4, y: 4, z: 8, core: 2. Of those that a mesh axis runs over, the one named last changes fastest.
Arguments:
- direct: bfloat16 [32, 512, 6144], P('freq', None, 'pts'), may hold values from -6 to 6
- onsets: int32 [32, 6144], P('freq', 'pts'), may hold values from 64 to 511
- left_bases: bfloat16 [128, 24, 24, 2, 8, 256], P('freq', 'pts'), may hold values from -0.4375 to 0.4375
- right_bases: bfloat16 [128, 24, 24, 2, 8, 256], P('freq', 'pts'), may hold values from -0.25 to 0.25
- tile_ranks: int32 [128, 24, 24], P('freq', 'pts'), may hold values from 1 to 8
Outputs:
- plus_field: float32 [32, 512, 6144], P('freq', None, 'pts')
- minus_field: float32 [32, 512, 6144], P('freq', None, 'pts')
The draws below stay inside these ranges and needn't reach their ends.
All inputs are finite; a program needn't handle non-finite values.
Results may differ from the reference program's by a relative error of at most 0.017.
Values may be sent and summed in bfloat16 or wider, within the bound.
A program may use at most 128 MiB of HBM per device.

```python
import math
import jax
import jax.numpy as jnp
from jax import lax

N = 6144
NB = 256
K = 8
F = 128
ITERS = 3
NT = 512
NTL = 24
P_SIZE = 32
N_PTS = 8


def place_ends(drawn, own_key, least, top_value):
    longest = drawn.shape.index(max(drawn.shape))
    spots = []
    for shift in (0, 1):
        where = [jax.random.randint(jax.random.fold_in(own_key, axis), (), 0, length) for axis, length in enumerate(drawn.shape)]
        where[longest] = (where[longest] + shift) % drawn.shape[longest]
        spots.append(tuple(where))
    return drawn.at[spots[0]].set(least).at[spots[1]].set(top_value)


def block_scale(stream_key, shape, shards, smallest, top_value):
    level = 1.0
    for position, parts in shards:
        steps = jax.random.uniform(jax.random.fold_in(jax.random.fold_in(stream_key, 6), position), (parts,), jnp.float32, smallest / len(shards), top_value / len(shards))
        level = level * jnp.repeat(jnp.exp(steps), shape[position] // parts).reshape((-1,) + (1,) * (len(shape) - 1 - position))
    return level


def gaussian(rng, dims, spread, most, cuts=(), dtype=jnp.bfloat16):
    array = spread * jax.random.normal(rng, dims, jnp.float32)
    if cuts:
        array = array * block_scale(rng, dims, cuts, -0.22, 0.18)
    return jnp.clip(array, -most, most).astype(dtype)


def setup_inputs(seed: int = 0) -> dict:
    seeds = jax.random.split(jax.random.key(seed), 6)
    return {
        "direct": gaussian(seeds[0], (P_SIZE, NT, N), 1.0, 6.0, ((0, 32), (2, 8))),
        "onsets": place_ends(jax.random.randint(seeds[1], (P_SIZE, N), NT // 8, NT), jax.random.fold_in(seeds[1], 1), NT // 8, NT - 1).astype(jnp.int32),
        "left_bases": gaussian(seeds[2], (F, NTL, NTL, 2, K, NB), (N // NB * K) ** -0.5, 0.4375, ((0, 32), (1, 8))),
        "right_bases": gaussian(seeds[3], (F, NTL, NTL, 2, K, NB), (2 * NB) ** -0.5, 0.25, ((0, 32), (1, 8))),
        "tile_ranks": place_ends(jax.random.randint(seeds[4], (F, NTL, NTL), 1, K + 1), jax.random.fold_in(seeds[4], 1), 1, K).astype(jnp.int32),
    }


HIGHEST = lax.Precision.HIGHEST

def band_tables(freq_total, sample_total):
    bins = lax.broadcasted_iota(jnp.int32, (freq_total, sample_total), 0) + 1
    moments = lax.broadcasted_iota(jnp.int32, (freq_total, sample_total), 1)
    phases = 2.0 * math.pi / sample_total * (bins * moments % sample_total).astype(jnp.float32)
    scaling = 1.0 / math.sqrt(sample_total)
    cosine = jnp.cos(phases) * scaling
    sine = jnp.sin(phases) * scaling
    return (jnp.stack([cosine, -sine]), jnp.stack([2.0 * cosine, -2.0 * sine]))

def rounded(values):
    return lax.optimization_barrier(values.astype(jnp.bfloat16)).astype(jnp.float32)

def contract(spec, left_part, right_part):
    return jnp.einsum(spec, left_part.astype(jnp.float32), right_part.astype(jnp.float32), precision=HIGHEST)

def conj_apply(spec, basis_real, basis_imag, vector_real, vector_imag):
    real_part = contract(spec, basis_real, vector_real) + contract(spec, basis_imag, vector_imag)
    imag_part = contract(spec, basis_real, vector_imag) - contract(spec, basis_imag, vector_real)
    return (real_part, imag_part)

def plain_apply(spec, basis_real, basis_imag, vector_real, vector_imag):
    real_part = contract(spec, basis_real, vector_real) - contract(spec, basis_imag, vector_imag)
    imag_part = contract(spec, basis_real, vector_imag) + contract(spec, basis_imag, vector_real)
    return (real_part, imag_part)

def reference(direct, onsets, left_bases, right_bases, tile_ranks):
    forward_exact, inverse_exact = band_tables(F, NT)
    forward_table = rounded(forward_exact)
    inverse_table = rounded(inverse_exact)
    point_total = direct.shape[0]
    tile_count = N // NB
    tile_group = tile_count // N_PTS
    moments = lax.broadcasted_iota(jnp.int32, direct.shape, 1)
    window = (moments < onsets[:, None, :]).astype(jnp.float32)
    rank_index = lax.broadcasted_iota(jnp.int32, tile_ranks.shape + (K,), 3)
    rank_mask = (rank_index < tile_ranks[..., None]).astype(jnp.float32)[..., None]

    def to_band(history):
        samples = rounded(history)
        spectrum = jnp.einsum('cft,ptn->cfpn', forward_table, samples, precision=HIGHEST)
        spectrum = spectrum.reshape(2, F, point_total, tile_count, NB).astype(jnp.bfloat16)
        return jnp.moveaxis(spectrum, 1, 0)

    def to_time(spectrum):
        flat = jnp.moveaxis(spectrum, 0, 1).reshape(2, F, point_total, N).astype(jnp.float32)
        return jnp.einsum('cft,cfpn->ptn', inverse_table, flat, precision=HIGHEST) * window

    def forward_one(operands):
        spectrum, left_part, right_part, mask_part = operands
        real_part, imag_part = conj_apply('ijkb,pjb->ijkp', right_part[:, :, 0], right_part[:, :, 1], spectrum[0], spectrum[1])
        terms = (jnp.stack([real_part, imag_part]) * mask_part).astype(jnp.bfloat16)
        real_part, imag_part = plain_apply('ijkb,ijkp->pib', left_part[:, :, 0], left_part[:, :, 1], terms[0], terms[1])
        return jnp.stack([real_part, imag_part]).astype(jnp.bfloat16)

    def adjoint_one(operands):
        spectrum, left_part, right_part, mask_part = operands
        real_part, imag_part = conj_apply('ijkb,pib->ijkp', left_part[:, :, 0], left_part[:, :, 1], spectrum[0], spectrum[1])
        terms = (jnp.stack([real_part, imag_part]) * mask_part).astype(jnp.bfloat16)
        terms = terms.reshape(2, N_PTS, tile_group, tile_count, K, point_total)
        grouped = right_part.reshape(N_PTS, tile_group, tile_count, 2, K, NB)
        real_part, imag_part = plain_apply('gijkb,gijkp->gpjb', grouped[:, :, :, 0], grouped[:, :, :, 1], terms[0], terms[1])
        partial_value = jnp.stack([real_part, imag_part], axis=1).astype(jnp.bfloat16)
        partial_value = lax.optimization_barrier(partial_value).astype(jnp.float32)
        return lax.optimization_barrier(jnp.sum(partial_value, axis=0)).astype(jnp.bfloat16)
    history = direct.astype(jnp.float32)
    plus_field = history
    minus_field = jnp.zeros_like(history)
    for iteration in range(ITERS):
        spectra = lax.map(forward_one, (to_band(history), left_bases, right_bases, rank_mask))
        reflected = to_time(spectra)
        minus_field = minus_field + reflected
        spectra = lax.map(adjoint_one, (to_band(reflected), left_bases, right_bases, rank_mask))
        history = to_time(spectra)
        plus_field = plus_field + history
    return (plus_field, minus_field)
```

```python
import functools
import math

import jax
import jax.numpy as jnp
import numpy as np
from jax import lax
from jax.experimental import pallas as pl
from jax.experimental.pallas import tpu as pltpu
from jax.sharding import PartitionSpec as P

NB = 256
K = 8
ITERS = 3
NZ = 8
MESH = pl.DeviceIdType.MESH
F32 = jnp.float32
BF16 = jnp.bfloat16


def band_tables(freq_total, sample_total):
    bins = np.arange(freq_total)[:, None] + 1
    moments = np.arange(sample_total)[None, :]
    phases = 2.0 * math.pi / sample_total * (bins * moments % sample_total)
    scaling = 1.0 / math.sqrt(sample_total)
    cosine = np.cos(phases) * scaling
    sine = np.sin(phases) * scaling
    forward = np.stack([cosine, -sine], axis=1).reshape(2 * freq_total, sample_total)
    inverse = np.stack([2.0 * cosine, -2.0 * sine], axis=1).reshape(2 * freq_total, sample_total).T
    return forward, inverse


def row_orders(inner, points):
    order = np.arange(inner * points).reshape(points, inner).T.reshape(-1)
    gather = np.eye(inner * points)[order]
    return gather, gather.T


def dot(left, right, dims=((1,), (0,))):
    return lax.dot_general(left, right, (dims, ((), ())), preferred_element_type=F32)


def spread(index, size):
    return size // 2 + (1 - 2 * lax.rem(index, 2)) * ((index + 1) // 2)


def kernel(
    ny,
    nz,
    npts,
    direct_ref,
    onsets_ref,
    left_ref,
    right_ref,
    ranks_ref,
    fwd_ref,
    inv_ref,
    gather_ref,
    scatter_ref,
    plus_ref,
    minus_ref,
    fields,
    base,
    left_raw,
    right_raw,
    send_f,
    recv_f,
    send_t,
    recv_t,
    send_p,
    recv_p,
    copy_sem,
    base_send,
    base_recv,
    fs_sem,
    fr_sem,
    ts_sem,
    tr_sem,
    ps_sem,
    pr_sem,
    fl_sem,
    tl_sem,
    pl_sem,
):
    nfreq = ny * nz
    tiles = 3
    ntl = npts * tiles
    fh = left_ref.shape[0]
    inner = 2 * fh
    nt = direct_ref.shape[0]
    me_f = lax.axis_index("freq")
    me_p = lax.axis_index("pts")
    my_y = me_f // nz
    my_z = lax.rem(me_f, nz)

    def freq_peer(n):
        dz = spread(n // ny, nz)
        dy = spread(lax.rem(n, ny), ny)
        return lax.rem(my_y + dy, ny) * nz + lax.rem(my_z + dz, nz)

    def pts_peer(n):
        return lax.rem(me_p + spread(n, npts), npts)

    barrier = pltpu.get_barrier_semaphore()

    def greet_f(n, c):
        pl.semaphore_signal(barrier, inc=1, device_id={"freq": freq_peer(n)}, device_id_type=MESH)
        return c

    def greet_p(n, c):
        pl.semaphore_signal(barrier, inc=1, device_id={"pts": pts_peer(n)}, device_id_type=MESH)
        return c

    lax.fori_loop(0, nfreq - 1, greet_f, 0)
    lax.fori_loop(0, npts - 1, greet_p, 0)

    left_copy = pltpu.make_async_copy(left_ref, left_raw, copy_sem.at[0])
    left_copy.start()

    def tile_cols(r):
        return pl.ds(pl.multiple_of(r * NB, NB), NB)

    def band(r, samples):
        spectrum = dot(fwd_ref[...], samples)
        send_f[r] = spectrum.reshape(nfreq, inner, NB).astype(BF16)

    def first_band(r, c):
        samples = direct_ref[:, tile_cols(r)]
        band(r, samples)
        fields[0, :, tile_cols(r)] = jnp.zeros((nt, NB), F32)
        fields[1, :, tile_cols(r)] = samples.astype(F32)
        return c

    lax.fori_loop(0, tiles, first_band, 0)
    pl.semaphore_wait(barrier, nfreq + npts - 2)

    def base_copy(q, source_q):
        return (right_ref.at[:, :, pl.ds(q * tiles, tiles)], right_raw.at[source_q])

    def send_base(n, c):
        q = pts_peer(n)
        src, dst = base_copy(q, me_p)
        pltpu.make_async_remote_copy(
            src, dst, base_send, base_recv, device_id={"pts": q}, device_id_type=MESH
        ).start()
        return c

    def exchange(r, send, recv, send_sem, recv_sem, local_sem):
        def one(n, c):
            d = freq_peer(n)
            pltpu.make_async_remote_copy(
                send.at[r, d],
                recv.at[r, me_f],
                send_sem.at[r],
                recv_sem.at[r],
                device_id={"freq": d},
                device_id_type=MESH,
            ).start()
            return c

        lax.fori_loop(0, nfreq - 1, one, 0)
        pltpu.make_async_copy(send.at[r, me_f], recv.at[r, me_f], local_sem.at[r]).start()

    def await_exchange(r, recv, recv_sem, local_sem):
        others = recv.at[r, pl.ds(0, nfreq - 1)]
        pltpu.make_async_copy(others, others, recv_sem.at[r]).wait()
        own = recv.at[r, me_f]
        pltpu.make_async_copy(own, own, local_sem.at[r]).wait()

    def await_sent(r, send, send_sem):
        others = send.at[r, pl.ds(0, nfreq - 1)]
        pltpu.make_async_copy(others, others, send_sem.at[r]).wait()

    def first_send(r, c):
        exchange(r, send_f, recv_f, fs_sem, fr_sem, fl_sem)
        return c

    lax.fori_loop(0, tiles, first_send, 0)
    lax.fori_loop(0, npts - 1, send_base, 0)
    own_src, own_dst = base_copy(me_p, me_p)
    own_base = pltpu.make_async_copy(own_src, own_dst, copy_sem.at[1])
    own_base.start()

    left_copy.wait()
    rank_row = lax.broadcasted_iota(jnp.int32, (K, NB), 0)

    def stack_left(i, c):
        f, a = i // tiles, lax.rem(i, tiles)
        for comp in range(2):
            rows = []
            for col in range(ntl):
                tile = left_raw[f, a, col, comp].astype(F32)
                rows.append(jnp.where(rank_row < ranks_ref[i, col], tile, 0.0))
            base[1, f, a, comp] = jnp.concatenate(rows, axis=0).astype(BF16)
        return c

    lax.fori_loop(0, fh * tiles, stack_left, 0)
    others = right_raw.at[pl.ds(0, npts - 1)]
    pltpu.make_async_copy(others, others, base_recv).wait()
    own_base.wait()

    def stack_right(i, c):
        f, col = i // tiles, lax.rem(i, tiles)
        for comp in range(2):
            block = right_raw[:, f, :, col, comp].astype(F32)
            base[0, f, col, comp] = block.reshape(ntl * K, NB).astype(BF16)
        return c

    lax.fori_loop(0, fh * tiles, stack_right, 0)

    def half_step(step, carry):
        side = lax.rem(step, 2)
        other = 1 - side

        def coefficients(r, c):
            await_exchange(r, recv_f, fr_sem, fl_sem)
            arrived = recv_f[r].astype(F32).reshape(nfreq * inner, NB).astype(BF16)
            spectrum = dot(gather_ref[...], arrived)
            rows = spectrum.astype(BF16)
            negated = (-spectrum).astype(BF16)
            blank = jnp.zeros((2 * nfreq, NB), BF16)

            @pl.when(step > 0)
            def _():
                sent = send_p.at[0, :, pl.ds(0, ntl - tiles)]
                pltpu.make_async_copy(sent, sent, ps_sem.at[r]).wait()

            for pair in range(fh // 2):
                total = None
                for half in range(2):
                    f = 2 * pair + half
                    lo, mid, hi = (2 * f) * nfreq, (2 * f + 1) * nfreq, (2 * f + 2) * nfreq
                    straight = rows[lo:hi]
                    turned = jnp.concatenate([rows[mid:hi], negated[lo:mid]], axis=0)
                    for comp, part in ((0, straight), (1, turned)):
                        parts = [part, blank] if half == 0 else [blank, part]
                        product = dot(
                            base[side, f, r, comp], jnp.concatenate(parts, axis=0), ((1,), (1,))
                        )
                        total = product if total is None else total + product
                send_p[r, pair] = total.reshape(ntl, K, 4 * nfreq).astype(BF16)

            def one(n, cc):
                q = pts_peer(n)
                pltpu.make_async_remote_copy(
                    send_p.at[r, :, pl.ds(q * tiles, tiles)],
                    recv_p.at[side, me_p * tiles + r],
                    ps_sem.at[r],
                    pr_sem.at[side],
                    device_id={"pts": q},
                    device_id_type=MESH,
                ).start()
                return cc

            lax.fori_loop(0, npts - 1, one, 0)
            own = pltpu.make_async_copy(
                send_p.at[r, :, pl.ds(me_p * tiles, tiles)],
                recv_p.at[side, me_p * tiles + r],
                pl_sem.at[r],
            )
            own.start()
            return c

        lax.fori_loop(0, tiles, coefficients, 0)
        arriving = recv_p.at[side, pl.ds(0, ntl - tiles)]
        pltpu.make_async_copy(arriving, arriving, pr_sem.at[side]).wait()
        for r in range(tiles):
            own = recv_p.at[side, me_p * tiles + r]
            pltpu.make_async_copy(own, own, pl_sem.at[r]).wait()

        def expand(r, c):
            blocks = []
            for pair in range(fh // 2):
                terms = recv_p[side, :, pair, r].astype(F32).reshape(ntl * K, 4 * nfreq)
                terms = jnp.transpose(terms)
                for half in range(2):
                    f = 2 * pair + half
                    real = terms[(2 * half) * nfreq : (2 * half + 1) * nfreq]
                    imag = terms[(2 * half + 1) * nfreq : (2 * half + 2) * nfreq]
                    straight = jnp.concatenate([real, imag], axis=0).astype(BF16)
                    turned = jnp.concatenate([-imag, real], axis=0).astype(BF16)
                    blocks.append(
                        dot(straight, base[other, f, r, 0]) + dot(turned, base[other, f, r, 1])
                    )
            spectrum = jnp.concatenate(blocks, axis=0).astype(BF16)
            ordered = dot(scatter_ref[...], spectrum)

            @pl.when(step > 0)
            def _():
                await_sent(r, send_t, ts_sem)

            send_t[r] = ordered.reshape(nfreq, inner, NB).astype(BF16)
            exchange(r, send_t, recv_t, ts_sem, tr_sem, tl_sem)
            return c

        lax.fori_loop(0, tiles, expand, 0)

        def samples(r, c):
            await_exchange(r, recv_t, tr_sem, tl_sem)
            arrived = recv_t[r].astype(F32).reshape(nfreq * inner, NB).astype(BF16)
            moments = lax.broadcasted_iota(jnp.int32, (nt, NB), 0)
            field = jnp.where(
                moments < onsets_ref[:, tile_cols(r)], dot(inv_ref[...], arrived), 0.0
            )

            @pl.when(step < 2 * ITERS - 1)
            def _():
                await_sent(r, send_f, fs_sem)
                band(r, field.astype(BF16))
                exchange(r, send_f, recv_f, fs_sem, fr_sem, fl_sem)

            fields[side, :, tile_cols(r)] += field
            return c

        lax.fori_loop(0, tiles, samples, 0)
        return carry

    lax.fori_loop(0, 2 * ITERS, half_step, 0)

    minus_out = pltpu.make_async_copy(fields.at[0], minus_ref, copy_sem.at[0])
    plus_out = pltpu.make_async_copy(fields.at[1], plus_ref, copy_sem.at[1])
    minus_out.start()
    plus_out.start()

    def drain(r, c):
        await_sent(r, send_f, fs_sem)
        await_sent(r, send_t, ts_sem)
        sent = send_p.at[0, :, pl.ds(0, ntl - tiles)]
        pltpu.make_async_copy(sent, sent, ps_sem.at[r]).wait()
        return c

    lax.fori_loop(0, tiles, drain, 0)
    sent = right_raw.at[pl.ds(0, npts - 1)]
    pltpu.make_async_copy(sent, sent, base_send).wait()
    minus_out.wait()
    plus_out.wait()


def body(ny, nz, npts, direct, onsets, left_bases, right_bases, tile_ranks):
    nfreq = ny * nz
    fh, tiles, ntl = left_bases.shape[:3]
    _, nt, cells = direct.shape
    freq_total = fh * nfreq
    inner = 2 * fh
    forward, inverse = band_tables(freq_total, nt)
    gather, scatter = row_orders(inner, nfreq)
    tables = [jnp.asarray(t, dtype=BF16) for t in (forward, inverse, gather, scatter)]
    vmem = pl.BlockSpec(memory_space=pltpu.VMEM)
    smem = pl.BlockSpec(memory_space=pltpu.SMEM)
    hbm = pl.BlockSpec(memory_space=pl.ANY)
    dma = pltpu.SemaphoreType.DMA
    slots = pltpu.VMEM((tiles, nfreq, inner, NB), BF16)
    field = jax.ShapeDtypeStruct((nt, cells), F32)
    plus_field, minus_field = pl.pallas_call(
        functools.partial(kernel, ny, nz, npts),
        out_shape=(field, field),
        in_specs=[vmem, vmem, hbm, hbm, smem, vmem, vmem, vmem, vmem],
        out_specs=(hbm, hbm),
        scratch_shapes=[
            pltpu.VMEM((2, nt, cells), F32),
            pltpu.VMEM((2, fh, tiles, 2, ntl * K, NB), BF16),
            pltpu.VMEM((fh, tiles, ntl, 2, K, NB), BF16),
            pltpu.VMEM((npts, fh, tiles, tiles, 2, K, NB), BF16),
            slots,
            slots,
            slots,
            slots,
            pltpu.VMEM((tiles, fh // 2, ntl, K, 4 * nfreq), BF16),
            pltpu.VMEM((2, ntl, fh // 2, tiles, K, 4 * nfreq), BF16),
            dma((2,)),
            dma,
            dma,
            dma((tiles,)),
            dma((tiles,)),
            dma((tiles,)),
            dma((tiles,)),
            dma((tiles,)),
            dma((2,)),
            dma((tiles,)),
            dma((tiles,)),
            dma((tiles,)),
        ],
        compiler_params=pltpu.CompilerParams(
            collective_id=0, has_side_effects=True, vmem_limit_bytes=56 * 1024 * 1024
        ),
    )(
        direct[0],
        onsets,
        left_bases,
        right_bases,
        tile_ranks.reshape(fh * tiles, ntl),
        *tables,
    )
    return plus_field[None], minus_field[None]


def solution(mesh):
    nfreq, npts = mesh.shape["freq"], mesh.shape["pts"]
    nz = NZ if nfreq % NZ == 0 and nfreq > NZ else 2
    return jax.shard_map(
        functools.partial(body, nfreq // nz, nz, npts),
        mesh=mesh,
        in_specs=(
            P("freq", None, "pts"),
            P("freq", "pts"),
            P("freq", "pts", None, None, None, None),
            P("freq", "pts", None, None, None, None),
            P("freq", "pts", None),
        ),
        out_specs=(P("freq", None, "pts"), P("freq", None, "pts")),
        check_vma=False,
    )
```

```python
import functools
import math

import jax
import jax.numpy as jnp
import numpy as np
from jax import lax
from jax.experimental import pallas as pl
from jax.experimental.pallas import tpu as pltpu
from jax.sharding import PartitionSpec as P

NB = 256
K = 8
ITERS = 3
NZ = 8
PAIR = 2
MESH = pl.DeviceIdType.MESH
F32 = jnp.float32
BF16 = jnp.bfloat16


def band_tables(freq_total, sample_total, owners):
    bins = np.arange(freq_total)[:, None] + 1
    moments = np.arange(sample_total)[None, :]
    phases = 2.0 * math.pi / sample_total * (bins * moments % sample_total)
    scaling = 1.0 / math.sqrt(sample_total)
    cosine = np.cos(phases) * scaling
    sine = np.sin(phases) * scaling

    def ordered(table):
        table = table.reshape(owners, freq_total // owners // PAIR, 2 * PAIR, sample_total)
        return np.moveaxis(table, 1, 0).reshape(2 * freq_total, sample_total)

    forward = ordered(np.stack([cosine, -sine], axis=1))
    inverse = ordered(np.stack([2.0 * cosine, -2.0 * sine], axis=1)).T
    return forward, inverse


def row_orders(inner, points):
    order = np.arange(inner * points).reshape(points, inner).T.reshape(-1)
    gather = np.eye(inner * points)[order]
    return gather, gather.T


def dot(left, right, dims=((1,), (0,))):
    return lax.dot_general(left, right, (dims, ((), ())), preferred_element_type=F32)


def spread(index, size):
    return size // 2 + (1 - 2 * (index % 2)) * ((index + 1) // 2)


def kernel(
    ny,
    nz,
    npts,
    direct_hbm,
    onsets_hbm,
    left_ref,
    right_hbm,
    ranks_ref,
    fwd_hbm,
    inv_hbm,
    gather_hbm,
    scatter_hbm,
    fields,
    direct_ref,
    onsets_ref,
    fwd_ref,
    inv_ref,
    gather_ref,
    scatter_ref,
    base,
    left_raw,
    right_ref,
    right_raw,
    send_f,
    recv_f,
    send_t,
    recv_t,
    send_p,
    recv_p,
    load_sem,
    base_send,
    base_recv,
    fs_sem,
    fr_sem,
    ts_sem,
    tr_sem,
    ps_sem,
    pr_sem,
):
    nfreq = ny * nz
    tiles = 3
    ntl = npts * tiles
    fh = left_ref.shape[0]
    pairs = fh // PAIR
    inner = 2 * PAIR
    nt = direct_ref.shape[0]
    me_f = lax.axis_index("freq")
    me_p = lax.axis_index("pts")
    my_y = me_f // nz
    my_z = lax.rem(me_f, nz)

    def freq_peer(n):
        y = lax.rem(my_y + spread(n % ny, ny), ny)
        z = lax.rem(my_z + spread(n // ny, nz), nz)
        return y * nz + z

    def pts_peer(n):
        return lax.rem(me_p + spread(n, npts), npts)

    barrier = pltpu.get_barrier_semaphore()
    for n in range(npts - 1):
        pl.semaphore_signal(barrier, inc=1, device_id={"pts": pts_peer(n)}, device_id_type=MESH)
    for n in range(nfreq - 1):
        pl.semaphore_signal(barrier, inc=1, device_id={"freq": freq_peer(n)}, device_id_type=MESH)

    loads = [
        pltpu.make_async_copy(src, dst, load_sem.at[i])
        for i, (src, dst) in enumerate(
            (
                (direct_hbm.at[0], direct_ref),
                (fwd_hbm, fwd_ref),
                (right_hbm, right_ref),
                (left_ref, left_raw),
                (inv_hbm, inv_ref),
                (gather_hbm, gather_ref),
                (scatter_hbm, scatter_ref),
                (onsets_hbm, onsets_ref),
            )
        )
    ]
    for load in loads:
        load.start()

    def tile_cols(r):
        return pl.ds(pl.multiple_of(r * NB, NB), NB)

    def band(r, samples):
        spectrum = dot(fwd_ref[...], samples)
        send_f[:, r] = spectrum.reshape(pairs, nfreq, inner, NB).astype(BF16)

    loads[0].wait()
    loads[1].wait()

    def first_band(r, c):
        band(r, direct_ref[:, tile_cols(r)])
        return c

    lax.fori_loop(0, tiles, first_band, 0)
    loads[2].wait()
    pl.semaphore_wait(barrier, nfreq + npts - 2)

    def await_all(ref, sem):
        pltpu.make_async_copy(ref, ref, sem).wait()

    def base_part(q, g):
        return right_ref.at[pl.ds(g * PAIR, PAIR), :, pl.ds(q * tiles, tiles)]

    for g in range(pairs):
        for n in range(npts - 1):
            q = pts_peer(n)
            pltpu.make_async_remote_copy(
                base_part(q, g),
                right_raw.at[g, me_p],
                base_send,
                base_recv.at[g],
                device_id={"pts": q},
                device_id_type=MESH,
            ).start()
        pltpu.make_async_copy(base_part(me_p, g), right_raw.at[g, me_p], base_recv.at[g]).start()

    def spectra_out(g, r):
        for n in range(nfreq - 1):
            d = freq_peer(n)
            pltpu.make_async_remote_copy(
                send_f.at[g, r, d],
                recv_f.at[g, r, me_f],
                fs_sem.at[r],
                fr_sem.at[g, r],
                device_id={"freq": d},
                device_id_type=MESH,
            ).start()
        pltpu.make_async_copy(
            send_f.at[g, r, me_f], recv_f.at[g, r, me_f], fr_sem.at[g, r]
        ).start()

    def first_send(i, c):
        spectra_out(i // tiles, lax.rem(i, tiles))
        return c

    lax.fori_loop(0, pairs * tiles, first_send, 0)

    def first_field(r, c):
        fields[0, :, tile_cols(r)] = jnp.zeros((nt, NB), F32)
        fields[1, :, tile_cols(r)] = direct_ref[:, tile_cols(r)].astype(F32)
        return c

    lax.fori_loop(0, tiles, first_field, 0)
    for load in loads[3:]:
        load.wait()

    rank_row = lax.broadcasted_iota(jnp.int32, (K, NB), 0)

    def stack_left(i, c):
        f, a = i // tiles, lax.rem(i, tiles)
        for comp in range(2):
            rows = []
            for col in range(ntl):
                tile = left_raw[f, a, col, comp].astype(F32)
                rows.append(jnp.where(rank_row < ranks_ref[a, f, col], tile, 0.0))
            base[1, f, a, comp] = jnp.concatenate(rows, axis=0).astype(BF16)
        return c

    lax.fori_loop(0, fh * tiles, stack_left, 0)

    def stack_right(g):
        await_all(right_raw.at[g], base_recv.at[g])

        def one(i, c):
            half, col = i // tiles, lax.rem(i, tiles)
            for comp in range(2):
                block = right_raw[g, :, half, :, col, comp].astype(F32)
                base[0, g * PAIR + half, col, comp] = block.reshape(ntl * K, NB).astype(BF16)
            return c

        lax.fori_loop(0, PAIR * tiles, one, 0)

    lanes = inner * nfreq

    def coefficients(step, g, r):
        side = lax.rem(step, 2)

        @pl.when((step == 0) & (r == 0))
        def _():
            stack_right(g)

        await_all(recv_f.at[g, r], fr_sem.at[g, r])
        arrived = recv_f[g, r].astype(F32).reshape(nfreq * inner, NB).astype(BF16)
        spectrum = dot(gather_ref[...], arrived)
        rows = spectrum.astype(BF16)
        negated = (-spectrum).astype(BF16)
        blank = jnp.zeros((lanes // PAIR, NB), BF16)

        @pl.when(step > 0)
        def _():
            await_all(send_p.at[g, 0, pl.ds(0, ntl - tiles)], ps_sem.at[g, r])

        total = None
        for half in range(PAIR):
            lo, mid, hi = (2 * half) * nfreq, (2 * half + 1) * nfreq, (2 * half + 2) * nfreq
            straight = rows[lo:hi]
            turned = jnp.concatenate([rows[mid:hi], negated[lo:mid]], axis=0)
            for comp, part in ((0, straight), (1, turned)):
                parts = [blank] * PAIR
                parts[half] = part
                product = dot(
                    base[side, g * PAIR + half, r, comp],
                    jnp.concatenate(parts, axis=0),
                    ((1,), (1,)),
                )
                total = product if total is None else total + product
        send_p[g, r] = total.reshape(ntl, K, lanes).astype(BF16)

        slot = recv_p.at[side, g, me_p * tiles + r]
        for n in range(npts - 1):
            q = pts_peer(n)
            pltpu.make_async_remote_copy(
                send_p.at[g, r, pl.ds(q * tiles, tiles)],
                slot,
                ps_sem.at[g, r],
                pr_sem.at[side, g],
                device_id={"pts": q},
                device_id_type=MESH,
            ).start()
        pltpu.make_async_copy(
            send_p.at[g, r, pl.ds(me_p * tiles, tiles)], slot, pr_sem.at[side, g]
        ).start()

    def expansion(step, g):
        side = lax.rem(step, 2)
        other = 1 - side
        await_all(recv_p.at[side, g], pr_sem.at[side, g])

        def expand(r, c):
            blocks = []
            terms = recv_p[side, g, :, r].astype(F32).reshape(ntl * K, lanes)
            terms = jnp.transpose(terms)
            for half in range(PAIR):
                lo, mid, hi = (2 * half) * nfreq, (2 * half + 1) * nfreq, (2 * half + 2) * nfreq
                real, imag = terms[lo:mid], terms[mid:hi]
                straight = terms[lo:hi].astype(BF16)
                turned = jnp.concatenate([-imag, real], axis=0).astype(BF16)
                f = g * PAIR + half
                blocks.append(
                    dot(straight, base[other, f, r, 0]) + dot(turned, base[other, f, r, 1])
                )
            ordered = dot(scatter_ref[...], jnp.concatenate(blocks, axis=0).astype(BF16))

            @pl.when(step > 0)
            def _():
                await_all(send_t.at[g, r, pl.ds(0, nfreq - 1)], ts_sem.at[g, r])

            send_t[g, r] = ordered.reshape(nfreq, inner, NB).astype(BF16)
            for n in range(nfreq - 1):
                d = freq_peer(n)
                pltpu.make_async_remote_copy(
                    send_t.at[g, r, d],
                    recv_t.at[r, g, me_f],
                    ts_sem.at[g, r],
                    tr_sem.at[r, g],
                    device_id={"freq": d},
                    device_id_type=MESH,
                ).start()
            pltpu.make_async_copy(
                send_t.at[g, r, me_f], recv_t.at[r, g, me_f], tr_sem.at[r, g]
            ).start()
            return c

        lax.fori_loop(0, tiles, expand, 0)

    def time_work(step):
        side = lax.rem(step, 2)
        last = 2 * ITERS - 1

        def samples(r, c):
            for g in range(pairs):
                await_all(recv_t.at[r, g], tr_sem.at[r, g])
            arrived = recv_t[r].astype(F32).reshape(pairs * nfreq * inner, NB).astype(BF16)
            moments = lax.broadcasted_iota(jnp.int32, (nt, NB), 0)
            field = jnp.where(
                moments < onsets_ref[:, tile_cols(r)], dot(inv_ref[...], arrived), 0.0
            )

            @pl.when(step < last)
            def _():
                await_all(send_f.at[:, r, pl.ds(0, nfreq - 1)], fs_sem.at[r])
                band(r, field.astype(BF16))
                spectra_out(0, r)

            fields[side, :, tile_cols(r)] += field
            return c

        lax.fori_loop(0, tiles, samples, 0)

        @pl.when(step < last)
        def _():
            def one(i, c):
                spectra_out(1 + i // tiles, lax.rem(i, tiles))
                return c

            lax.fori_loop(0, (pairs - 1) * tiles, one, 0)

    def half_step(step, carry):
        count = 3 + 3 * jnp.minimum(step, 1)

        def pair_work(g, c):
            def one(i, cc):
                coefficients(step, i // tiles, lax.rem(i, tiles))
                return cc

            lax.fori_loop(g * count, count + g * (pairs * tiles - count), one, 0)
            expansion(step, g)
            return c

        lax.fori_loop(0, pairs, pair_work, 0)
        time_work(step)
        return carry

    lax.fori_loop(0, 2 * ITERS, half_step, 0)

    def drain(r, c):
        await_all(send_f.at[:, r, pl.ds(0, nfreq - 1)], fs_sem.at[r])
        for g in range(pairs):
            await_all(send_t.at[g, r, pl.ds(0, nfreq - 1)], ts_sem.at[g, r])
            await_all(send_p.at[g, 0, pl.ds(0, ntl - tiles)], ps_sem.at[g, r])
        return c

    lax.fori_loop(0, tiles, drain, 0)
    await_all(right_raw.at[:, pl.ds(0, npts - 1)], base_send)


def body(ny, nz, npts, direct, onsets, left_bases, right_bases, tile_ranks):
    nfreq = ny * nz
    fh, tiles, ntl = left_bases.shape[:3]
    _, nt, cells = direct.shape
    pairs = fh // PAIR
    inner = 2 * PAIR
    forward, inverse = band_tables(fh * nfreq, nt, nfreq)
    gather, scatter = row_orders(inner, nfreq)
    tables = [jnp.asarray(t, dtype=BF16) for t in (forward, inverse, gather, scatter)]
    smem = pl.BlockSpec(memory_space=pltpu.SMEM)
    hbm = pl.BlockSpec(memory_space=pl.ANY)
    dma = pltpu.SemaphoreType.DMA

    def in_hbm(array):
        return pltpu.with_memory_space_constraint(array, pltpu.HBM)

    fields = pl.pallas_call(
        functools.partial(kernel, ny, nz, npts),
        out_shape=jax.ShapeDtypeStruct((2, nt, cells), F32),
        in_specs=[hbm, hbm, hbm, hbm, smem, hbm, hbm, hbm, hbm],
        out_specs=pl.BlockSpec(memory_space=pltpu.VMEM),
        scratch_shapes=[
            pltpu.VMEM((nt, cells), BF16),
            pltpu.VMEM((1, cells), jnp.int32),
            *[pltpu.VMEM(t.shape, BF16) for t in tables],
            pltpu.VMEM((2, fh, tiles, 2, ntl * K, NB), BF16),
            pltpu.VMEM((fh, tiles, ntl, 2, K, NB), BF16),
            pltpu.VMEM((fh, tiles, ntl, 2, K, NB), BF16),
            pltpu.VMEM((pairs, npts, PAIR, tiles, tiles, 2, K, NB), BF16),
            pltpu.VMEM((pairs, tiles, nfreq, inner, NB), BF16),
            pltpu.VMEM((pairs, tiles, nfreq, inner, NB), BF16),
            pltpu.VMEM((pairs, tiles, nfreq, inner, NB), BF16),
            pltpu.VMEM((tiles, pairs, nfreq, inner, NB), BF16),
            pltpu.VMEM((pairs, tiles, ntl, K, inner * nfreq), BF16),
            pltpu.VMEM((2, pairs, ntl, tiles, K, inner * nfreq), BF16),
            dma((8,)),
            dma,
            dma((pairs,)),
            dma((tiles,)),
            dma((pairs, tiles)),
            dma((pairs, tiles)),
            dma((tiles, pairs)),
            dma((pairs, tiles)),
            dma((2, pairs)),
        ],
        compiler_params=pltpu.CompilerParams(
            collective_id=0, has_side_effects=True, vmem_limit_bytes=32 * 1024 * 1024
        ),
    )(
        in_hbm(direct),
        in_hbm(onsets),
        in_hbm(left_bases),
        in_hbm(right_bases),
        jnp.transpose(tile_ranks, (1, 0, 2)),
        *[in_hbm(t) for t in tables],
    )
    return fields[1:], fields[:1]


def solution(mesh):
    nfreq, npts = mesh.shape["freq"], mesh.shape["pts"]
    nz = NZ if nfreq > NZ else 4
    return jax.shard_map(
        functools.partial(body, nfreq // nz, nz, npts),
        mesh=mesh,
        in_specs=(
            P("freq", None, "pts"),
            P("freq", "pts"),
            P("freq", "pts", None, None, None, None),
            P("freq", "pts", None, None, None, None),
            P("freq", "pts", None),
        ),
        out_specs=(P("freq", None, "pts"), P("freq", None, "pts")),
        check_vma=False,
    )
```

```python
import functools
import math

import jax
import jax.numpy as jnp
import numpy as np
from jax import lax
from jax.experimental import pallas as pl
from jax.experimental.pallas import tpu as pltpu
from jax.sharding import PartitionSpec as P

NB = 256
K = 8
ITERS = 3
NZ = 8
PAIR = 2
MESH = pl.DeviceIdType.MESH
F32 = jnp.float32
BF16 = jnp.bfloat16


def band_tables(freq_total, sample_total, owners):
    bins = np.arange(freq_total)[:, None] + 1
    moments = np.arange(sample_total)[None, :]
    phases = 2.0 * math.pi / sample_total * (bins * moments % sample_total)
    scaling = 1.0 / math.sqrt(sample_total)
    cosine = np.cos(phases) * scaling
    sine = np.sin(phases) * scaling

    def ordered(table):
        table = table.reshape(owners, freq_total // owners // PAIR, 2 * PAIR, sample_total)
        return np.moveaxis(table, 1, 0).reshape(2 * freq_total, sample_total)

    forward = ordered(np.stack([cosine, -sine], axis=1))
    inverse = ordered(np.stack([2.0 * cosine, -2.0 * sine], axis=1)).T
    return forward, inverse


def row_orders(inner, points):
    order = np.arange(inner * points).reshape(points, inner).T.reshape(-1)
    gather = np.eye(inner * points)[order]
    return gather, gather.T


def dot(left, right, dims=((1,), (0,))):
    return lax.dot_general(left, right, (dims, ((), ())), preferred_element_type=F32)


def spread(index, size):
    return size // 2 + (1 - 2 * (index % 2)) * ((index + 1) // 2)


def kernel(
    ny,
    nz,
    npts,
    direct_hbm,
    onsets_hbm,
    left_ref,
    right_ref,
    ranks_hbm,
    fwd_hbm,
    inv_hbm,
    gather_hbm,
    scatter_hbm,
    fields,
    direct_ref,
    onsets_ref,
    ranks_ref,
    fwd_ref,
    inv_ref,
    gather_ref,
    scatter_ref,
    base,
    left_raw,
    right_raw,
    send_f,
    recv_f,
    send_t,
    recv_t,
    send_p,
    recv_p,
    load_sem,
    base_send,
    base_recv,
    fs_sem,
    fr_sem,
    ts_sem,
    tr_sem,
    ps_sem,
    pr_sem,
):
    nfreq = ny * nz
    tiles = 3
    ntl = npts * tiles
    fh = left_ref.shape[0]
    pairs = fh // PAIR
    inner = 2 * PAIR
    nt = direct_ref.shape[0]
    me_f = lax.axis_index("freq")
    me_p = lax.axis_index("pts")
    my_y = me_f // nz
    my_z = lax.rem(me_f, nz)

    offsets = [(dy, dz) for dz in range(nz) for dy in range(ny)]
    offsets.sort(key=lambda o: (-min(o[0], ny - o[0]) - min(o[1], nz - o[1]), o[0], o[1]))

    def freq_peer(n):
        dy, dz = offsets[n]
        return lax.rem(my_y + dy, ny) * nz + lax.rem(my_z + dz, nz)

    def pts_peer(n):
        return lax.rem(me_p + spread(n, npts), npts)

    barrier = pltpu.get_barrier_semaphore()
    for n in range(npts - 1):
        pl.semaphore_signal(barrier, inc=1, device_id={"pts": pts_peer(n)}, device_id_type=MESH)
    for n in range(nfreq - 1):
        pl.semaphore_signal(barrier, inc=1, device_id={"freq": freq_peer(n)}, device_id_type=MESH)

    loads = [
        pltpu.make_async_copy(src, dst, load_sem.at[i])
        for i, (src, dst) in enumerate(
            (
                (direct_hbm.at[0], direct_ref),
                (fwd_hbm, fwd_ref),
                (left_ref, left_raw),
                (inv_hbm, inv_ref),
                (gather_hbm, gather_ref),
                (scatter_hbm, scatter_ref),
                (onsets_hbm, onsets_ref),
                (ranks_hbm, ranks_ref),
            )
        )
    ]
    for load in loads:
        load.start()

    def tile_cols(r):
        return pl.ds(pl.multiple_of(r * NB, NB), NB)

    def band(r, samples):
        spectrum = dot(fwd_ref[...], samples)
        send_f[:, r] = spectrum.reshape(pairs, nfreq, inner, NB).astype(BF16)

    pl.semaphore_wait(barrier, nfreq + npts - 2)

    def await_all(ref, sem):
        pltpu.make_async_copy(ref, ref, sem).wait()

    def base_part(q, g, r):
        return right_ref.at[pl.ds(g * PAIR, PAIR), :, pl.ds(q * tiles + r, 1)]

    def base_out(i, c):
        g, r = i // tiles, lax.rem(i, tiles)
        for n in range(npts - 1):
            q = pts_peer(n)
            pltpu.make_async_remote_copy(
                base_part(q, g, r),
                right_raw.at[g, r, me_p],
                base_send,
                base_recv.at[g, r],
                device_id={"pts": q},
                device_id_type=MESH,
            ).start()
        pltpu.make_async_copy(
            base_part(me_p, g, r), right_raw.at[g, r, me_p], base_recv.at[g, r]
        ).start()
        return c

    lax.fori_loop(0, pairs * tiles, base_out, 0)
    loads[0].wait()
    loads[1].wait()

    def first_band(r, c):
        band(r, direct_ref[:, tile_cols(r)])
        return c

    lax.fori_loop(0, tiles, first_band, 0)

    def spectra_out(g, r):
        for n in range(nfreq - 1):
            d = freq_peer(n)
            pltpu.make_async_remote_copy(
                send_f.at[g, r, d],
                recv_f.at[g, r, me_f],
                fs_sem.at[r],
                fr_sem.at[g, r],
                device_id={"freq": d},
                device_id_type=MESH,
            ).start()
        pltpu.make_async_copy(
            send_f.at[g, r, me_f], recv_f.at[g, r, me_f], fr_sem.at[g, r]
        ).start()

    def first_send(i, c):
        spectra_out(i // tiles, lax.rem(i, tiles))
        return c

    lax.fori_loop(0, pairs * tiles, first_send, 0)

    def first_field(r, c):
        fields[0, :, tile_cols(r)] = jnp.zeros((nt, NB), F32)
        fields[1, :, tile_cols(r)] = direct_ref[:, tile_cols(r)].astype(F32)
        return c

    lax.fori_loop(0, tiles, first_field, 0)
    for load in loads[2:]:
        load.wait()

    rank_row = lax.broadcasted_iota(jnp.int32, (K, NB), 0)

    def stack_left(i, c):
        f, a = i // tiles, lax.rem(i, tiles)
        for comp in range(2):
            rows = []
            for col in range(ntl):
                tile = left_raw[f, a, col, comp].astype(F32)
                rows.append(jnp.where(rank_row < ranks_ref[a, f, col], tile, 0.0))
            base[1, f, a, comp] = jnp.concatenate(rows, axis=0).astype(BF16)
        return c

    lax.fori_loop(0, fh * tiles, stack_left, 0)

    def stack_right(g, r):
        await_all(right_raw.at[g, r], base_recv.at[g, r])
        for half in range(PAIR):
            for comp in range(2):
                block = right_raw[g, r, :, half, :, 0, comp].astype(F32)
                base[0, g * PAIR + half, r, comp] = block.reshape(ntl * K, NB).astype(BF16)

    lanes = inner * nfreq

    def coefficients(step, g, r):
        side = lax.rem(step, 2)

        @pl.when(step == 0)
        def _():
            stack_right(g, r)

        await_all(recv_f.at[g, r], fr_sem.at[g, r])
        arrived = recv_f[g, r].astype(F32).reshape(nfreq * inner, NB).astype(BF16)
        spectrum = dot(gather_ref[...], arrived)
        rows = spectrum.astype(BF16)
        negated = (-spectrum).astype(BF16)
        blank = jnp.zeros((lanes // PAIR, NB), BF16)

        @pl.when(step > 0)
        def _():
            await_all(send_p.at[g, 0, pl.ds(0, ntl - tiles)], ps_sem.at[g, r])

        total = None
        for half in range(PAIR):
            lo, mid, hi = (2 * half) * nfreq, (2 * half + 1) * nfreq, (2 * half + 2) * nfreq
            straight = rows[lo:hi]
            turned = jnp.concatenate([rows[mid:hi], negated[lo:mid]], axis=0)
            for comp, part in ((0, straight), (1, turned)):
                parts = [blank] * PAIR
                parts[half] = part
                product = dot(
                    base[side, g * PAIR + half, r, comp],
                    jnp.concatenate(parts, axis=0),
                    ((1,), (1,)),
                )
                total = product if total is None else total + product
        send_p[g, r] = total.reshape(ntl, K, lanes).astype(BF16)

        slot = recv_p.at[side, g, me_p * tiles + r]
        for n in range(npts - 1):
            q = pts_peer(n)
            pltpu.make_async_remote_copy(
                send_p.at[g, r, pl.ds(q * tiles, tiles)],
                slot,
                ps_sem.at[g, r],
                pr_sem.at[side, g],
                device_id={"pts": q},
                device_id_type=MESH,
            ).start()
        pltpu.make_async_copy(
            send_p.at[g, r, pl.ds(me_p * tiles, tiles)], slot, pr_sem.at[side, g]
        ).start()

    def results_out(g, r):
        for n in range(nfreq - 1):
            d = freq_peer(n)
            pltpu.make_async_remote_copy(
                send_t.at[g, r, d],
                recv_t.at[r, g, me_f],
                ts_sem.at[g, r],
                tr_sem.at[r, g],
                device_id={"freq": d},
                device_id_type=MESH,
            ).start()
        pltpu.make_async_copy(
            send_t.at[g, r, me_f], recv_t.at[r, g, me_f], tr_sem.at[r, g]
        ).start()

    def expansion(step, g):
        side = lax.rem(step, 2)
        other = 1 - side
        await_all(recv_p.at[side, g], pr_sem.at[side, g])

        def expand(r, c):
            blocks = []
            terms = recv_p[side, g, :, r].astype(F32).reshape(ntl * K, lanes)
            terms = jnp.transpose(terms)
            for half in range(PAIR):
                lo, mid, hi = (2 * half) * nfreq, (2 * half + 1) * nfreq, (2 * half + 2) * nfreq
                real, imag = terms[lo:mid], terms[mid:hi]
                straight = terms[lo:hi].astype(BF16)
                turned = jnp.concatenate([-imag, real], axis=0).astype(BF16)
                f = g * PAIR + half
                blocks.append(
                    dot(straight, base[other, f, r, 0]) + dot(turned, base[other, f, r, 1])
                )
            ordered = dot(scatter_ref[...], jnp.concatenate(blocks, axis=0).astype(BF16))

            @pl.when(step > 0)
            def _():
                await_all(send_t.at[g, r, pl.ds(0, nfreq - 1)], ts_sem.at[g, r])

            send_t[g, r] = ordered.reshape(nfreq, inner, NB).astype(BF16)

            @pl.when((g > 0) | (r < tiles - 1))
            def _():
                results_out(g, r)

            @pl.when((g == 1) & (r == tiles - 2))
            def _():
                results_out(0, tiles - 1)

            return c

        lax.fori_loop(0, tiles, expand, 0)

    def time_work(step):
        side = lax.rem(step, 2)
        last = 2 * ITERS - 1

        def samples(r, c):
            for g in range(pairs):
                await_all(recv_t.at[r, g], tr_sem.at[r, g])
            arrived = recv_t[r].astype(F32).reshape(pairs * nfreq * inner, NB).astype(BF16)
            moments = lax.broadcasted_iota(jnp.int32, (nt, NB), 0)
            field = jnp.where(
                moments < onsets_ref[:, tile_cols(r)], dot(inv_ref[...], arrived), 0.0
            )

            @pl.when(step < last)
            def _():
                await_all(send_f.at[:, r, pl.ds(0, nfreq - 1)], fs_sem.at[r])
                band(r, field.astype(BF16))
                spectra_out(0, r)

            @pl.when((step < last) & (r == tiles - 2))
            def _():
                spectra_out(1, 0)

            fields[side, :, tile_cols(r)] += field
            return c

        lax.fori_loop(0, tiles, samples, 0)

        @pl.when(step < last)
        def _():
            def one(r, c):
                spectra_out(1, r)
                return c

            lax.fori_loop(1, tiles, one, 0)

    def half_step(step, carry):
        def one(i, c):
            order = jnp.where(i == 2, 3, jnp.where(i == 3, 2, i))
            coefficients(step, order // tiles, lax.rem(order, tiles))
            return c

        def two(g, c):
            expansion(step, g)
            return c

        lax.fori_loop(0, pairs * tiles, one, 0)
        lax.fori_loop(0, pairs, two, 0)
        time_work(step)
        return carry

    lax.fori_loop(0, 2 * ITERS, half_step, 0)

    def drain(r, c):
        await_all(send_f.at[:, r, pl.ds(0, nfreq - 1)], fs_sem.at[r])
        for g in range(pairs):
            await_all(send_t.at[g, r, pl.ds(0, nfreq - 1)], ts_sem.at[g, r])
            await_all(send_p.at[g, 0, pl.ds(0, ntl - tiles)], ps_sem.at[g, r])
        return c

    lax.fori_loop(0, tiles, drain, 0)
    await_all(right_raw.at[:, :, pl.ds(0, npts - 1)], base_send)


def body(ny, nz, npts, direct, onsets, left_bases, right_bases, tile_ranks):
    nfreq = ny * nz
    fh, tiles, ntl = left_bases.shape[:3]
    _, nt, cells = direct.shape
    pairs = fh // PAIR
    inner = 2 * PAIR
    forward, inverse = band_tables(fh * nfreq, nt, nfreq)
    gather, scatter = row_orders(inner, nfreq)
    tables = [jnp.asarray(t, dtype=BF16) for t in (forward, inverse, gather, scatter)]
    hbm = pl.BlockSpec(memory_space=pl.ANY)
    dma = pltpu.SemaphoreType.DMA

    def in_hbm(array):
        return pltpu.with_memory_space_constraint(array, pltpu.HBM)

    fields = pl.pallas_call(
        functools.partial(kernel, ny, nz, npts),
        out_shape=jax.ShapeDtypeStruct((2, nt, cells), F32),
        in_specs=[hbm] * 9,
        out_specs=pl.BlockSpec(memory_space=pltpu.VMEM),
        scratch_shapes=[
            pltpu.VMEM((nt, cells), BF16),
            pltpu.VMEM((1, cells), jnp.int32),
            pltpu.SMEM((tiles, fh, ntl), jnp.int32),
            *[pltpu.VMEM(t.shape, BF16) for t in tables],
            pltpu.VMEM((2, fh, tiles, 2, ntl * K, NB), BF16),
            pltpu.VMEM((fh, tiles, ntl, 2, K, NB), BF16),
            pltpu.VMEM((pairs, tiles, npts, PAIR, tiles, 1, 2, K, NB), BF16),
            pltpu.VMEM((pairs, tiles, nfreq, inner, NB), BF16),
            pltpu.VMEM((pairs, tiles, nfreq, inner, NB), BF16),
            pltpu.VMEM((pairs, tiles, nfreq, inner, NB), BF16),
            pltpu.VMEM((tiles, pairs, nfreq, inner, NB), BF16),
            pltpu.VMEM((pairs, tiles, ntl, K, inner * nfreq), BF16),
            pltpu.VMEM((2, pairs, ntl, tiles, K, inner * nfreq), BF16),
            dma((8,)),
            dma,
            dma((pairs, tiles)),
            dma((tiles,)),
            dma((pairs, tiles)),
            dma((pairs, tiles)),
            dma((tiles, pairs)),
            dma((pairs, tiles)),
            dma((2, pairs)),
        ],
        compiler_params=pltpu.CompilerParams(
            collective_id=0, has_side_effects=True, vmem_limit_bytes=32 * 1024 * 1024
        ),
    )(
        in_hbm(direct),
        in_hbm(onsets),
        in_hbm(left_bases),
        in_hbm(right_bases),
        in_hbm(jnp.transpose(tile_ranks, (1, 0, 2))),
        *[in_hbm(t) for t in tables],
    )
    return fields[1:], fields[:1]


def solution(mesh):
    nfreq, npts = mesh.shape["freq"], mesh.shape["pts"]
    nz = NZ if nfreq > NZ else 4
    return jax.shard_map(
        functools.partial(body, nfreq // nz, nz, npts),
        mesh=mesh,
        in_specs=(
            P("freq", None, "pts"),
            P("freq", "pts"),
            P("freq", "pts", None, None, None, None),
            P("freq", "pts", None, None, None, None),
            P("freq", "pts", None),
        ),
        out_specs=(P("freq", None, "pts"), P("freq", None, "pts")),
        check_vma=False,
    )
```

```python
import functools
import math

import jax
import jax.numpy as jnp
import numpy as np
from jax import lax
from jax.experimental import pallas as pl
from jax.experimental.pallas import tpu as pltpu
from jax.sharding import PartitionSpec as P

NB = 256
K = 8
ITERS = 3
NZ = 8
PAIR = 2
MESH = pl.DeviceIdType.MESH
F32 = jnp.float32
BF16 = jnp.bfloat16


def band_tables(freq_total, sample_total, owners):
    bins = np.arange(freq_total)[:, None] + 1
    moments = np.arange(sample_total)[None, :]
    phases = 2.0 * math.pi / sample_total * (bins * moments % sample_total)
    scaling = 1.0 / math.sqrt(sample_total)
    cosine = np.cos(phases) * scaling
    sine = np.sin(phases) * scaling

    def ordered(table):
        table = table.reshape(owners, freq_total // owners // PAIR, 2 * PAIR, sample_total)
        return np.moveaxis(table, 1, 0).reshape(2 * freq_total, sample_total)

    forward = ordered(np.stack([cosine, -sine], axis=1))
    inverse = ordered(np.stack([2.0 * cosine, -2.0 * sine], axis=1)).T
    return forward, inverse


def dot(left, right, dims=((1,), (0,))):
    return lax.dot_general(left, right, (dims, ((), ())), preferred_element_type=F32)


def spread(index, size):
    return size // 2 + (1 - 2 * (index % 2)) * ((index + 1) // 2)


def kernel(
    ny,
    nz,
    npts,
    direct_hbm,
    onsets_hbm,
    left_ref,
    right_ref,
    ranks_hbm,
    fwd_hbm,
    inv_hbm,
    fields,
    direct_ref,
    onsets_ref,
    ranks_ref,
    fwd_ref,
    inv_ref,
    base,
    left_raw,
    right_raw,
    send_f,
    recv_f,
    send_t,
    recv_t,
    send_p,
    recv_p,
    load_sem,
    base_send,
    base_recv,
    fs_sem,
    fr_sem,
    ts_sem,
    tr_sem,
    ps_sem,
    pr_sem,
):
    nfreq = ny * nz
    tiles = 3
    ntl = npts * tiles
    fh = left_ref.shape[0]
    pairs = fh // PAIR
    inner = 2 * PAIR
    nt = direct_ref.shape[0]
    me_f = lax.axis_index("freq")
    me_p = lax.axis_index("pts")
    my_y = me_f // nz
    my_z = lax.rem(me_f, nz)

    offsets = [(dy, dz) for dz in range(nz) for dy in range(ny)]
    offsets.sort(key=lambda o: (-min(o[0], ny - o[0]) - min(o[1], nz - o[1]), o[0], o[1]))

    def freq_peer(n):
        dy, dz = offsets[n]
        return lax.rem(my_y + dy, ny) * nz + lax.rem(my_z + dz, nz)

    def pts_peer(n):
        return lax.rem(me_p + spread(n, npts), npts)

    barrier = pltpu.get_barrier_semaphore()
    for n in range(npts - 1):
        pl.semaphore_signal(barrier, inc=1, device_id={"pts": pts_peer(n)}, device_id_type=MESH)
    for n in range(nfreq - 1):
        pl.semaphore_signal(barrier, inc=1, device_id={"freq": freq_peer(n)}, device_id_type=MESH)

    loads = [
        pltpu.make_async_copy(src, dst, load_sem.at[i])
        for i, (src, dst) in enumerate(
            (
                (direct_hbm.at[0], direct_ref),
                (fwd_hbm, fwd_ref),
                (left_ref, left_raw),
                (inv_hbm, inv_ref),
                (onsets_hbm, onsets_ref),
                (ranks_hbm, ranks_ref),
            )
        )
    ]
    for load in loads:
        load.start()

    def tile_cols(r):
        return pl.ds(pl.multiple_of(r * NB, NB), NB)

    def band(g, r, samples):
        rows = nfreq * inner
        spectrum = dot(fwd_ref[g * rows : (g + 1) * rows], samples)
        send_f[g, r] = spectrum.reshape(nfreq, inner, NB).astype(BF16)

    pl.semaphore_wait(barrier, nfreq + npts - 2)

    def await_all(ref, sem):
        pltpu.make_async_copy(ref, ref, sem).wait()

    def base_part(q, g, r):
        return right_ref.at[pl.ds(g * PAIR, PAIR), :, pl.ds(q * tiles + r, 1)]

    def base_out(i, c):
        g, r = i // tiles, lax.rem(i, tiles)
        for n in range(npts - 1):
            q = pts_peer(n)
            pltpu.make_async_remote_copy(
                base_part(q, g, r),
                right_raw.at[g, r, me_p],
                base_send,
                base_recv.at[g, r],
                device_id={"pts": q},
                device_id_type=MESH,
            ).start()
        pltpu.make_async_copy(
            base_part(me_p, g, r), right_raw.at[g, r, me_p], base_recv.at[g, r]
        ).start()
        return c

    lax.fori_loop(0, pairs * tiles, base_out, 0)
    loads[0].wait()
    loads[1].wait()

    def first_band(r, c):
        for g in range(pairs):
            band(g, r, direct_ref[:, tile_cols(r)])
        return c

    lax.fori_loop(0, tiles, first_band, 0)

    def spectra_out(g, r):
        for n in range(nfreq - 1):
            d = freq_peer(n)
            pltpu.make_async_remote_copy(
                send_f.at[g, r, d],
                recv_f.at[g, r, me_f],
                fs_sem.at[r],
                fr_sem.at[g, r],
                device_id={"freq": d},
                device_id_type=MESH,
            ).start()
        pltpu.make_async_copy(
            send_f.at[g, r, me_f], recv_f.at[g, r, me_f], fr_sem.at[g, r]
        ).start()

    def first_send(i, c):
        spectra_out(i // tiles, lax.rem(i, tiles))
        return c

    lax.fori_loop(0, pairs * tiles, first_send, 0)

    def first_field(r, c):
        fields[0, :, tile_cols(r)] = jnp.zeros((nt, NB), F32)
        fields[1, :, tile_cols(r)] = direct_ref[:, tile_cols(r)].astype(F32)
        return c

    lax.fori_loop(0, tiles, first_field, 0)
    for load in loads[2:]:
        load.wait()

    rank_row = lax.broadcasted_iota(jnp.int32, (K, NB), 0)

    def stack_left(i, c):
        f, a = i // tiles, lax.rem(i, tiles)
        for comp in range(2):
            rows = []
            for col in range(ntl):
                tile = left_raw[f, a, col, comp].astype(F32)
                rows.append(jnp.where(rank_row < ranks_ref[a, f, col], tile, 0.0))
            base[1, f, a, comp] = jnp.concatenate(rows, axis=0).astype(BF16)
        return c

    lax.fori_loop(0, fh * tiles, stack_left, 0)

    def stack_right(g, r):
        await_all(right_raw.at[g, r], base_recv.at[g, r])
        for half in range(PAIR):
            for comp in range(2):
                block = right_raw[g, r, :, half, :, 0, comp].astype(F32)
                base[0, g * PAIR + half, r, comp] = block.reshape(ntl * K, NB).astype(BF16)

    lanes = inner * nfreq

    def row_of(width):
        return lax.broadcasted_iota(jnp.int32, (lanes, width), 0)

    def bin_row(width):
        return lax.rem(row_of(width), inner) // 2

    def swapped(values, sign):
        width = values.shape[1]
        after = pltpu.roll(values, lanes - 1, 0)
        before = pltpu.roll(values, 1, 0)
        even = lax.rem(row_of(width), 2) == 0
        return jnp.where(even, sign * after, -sign * before)

    def coefficients(step, g, r):
        side = lax.rem(step, 2)

        @pl.when(step == 0)
        def _():
            stack_right(g, r)

        await_all(recv_f.at[g, r], fr_sem.at[g, r])
        arrived = recv_f[g, r].astype(F32).reshape(lanes, NB)
        turned = swapped(arrived, 1.0)

        @pl.when(step > 0)
        def _():
            await_all(send_p.at[g, 0, pl.ds(0, ntl - tiles)], ps_sem.at[g, r])

        total = None
        for half in range(PAIR):
            here = bin_row(NB) == half
            for comp, part in ((0, arrived), (1, turned)):
                product = dot(
                    base[side, g * PAIR + half, r, comp],
                    jnp.where(here, part, 0.0).astype(BF16),
                    ((1,), (1,)),
                )
                total = product if total is None else total + product
        send_p[g, r] = total.reshape(ntl, K, lanes).astype(BF16)

        slot = recv_p.at[side, g, me_p * tiles + r]
        for n in range(npts - 1):
            q = pts_peer(n)
            pltpu.make_async_remote_copy(
                send_p.at[g, r, pl.ds(q * tiles, tiles)],
                slot,
                ps_sem.at[g, r],
                pr_sem.at[side, g],
                device_id={"pts": q},
                device_id_type=MESH,
            ).start()
        pltpu.make_async_copy(
            send_p.at[g, r, pl.ds(me_p * tiles, tiles)], slot, pr_sem.at[side, g]
        ).start()

    def results_out(g, r):
        for n in range(nfreq - 1):
            d = freq_peer(n)
            pltpu.make_async_remote_copy(
                send_t.at[g, r, d],
                recv_t.at[r, g, me_f],
                ts_sem.at[g, r],
                tr_sem.at[r, g],
                device_id={"freq": d},
                device_id_type=MESH,
            ).start()
        pltpu.make_async_copy(
            send_t.at[g, r, me_f], recv_t.at[r, g, me_f], tr_sem.at[r, g]
        ).start()

    def expansion(step, g):
        side = lax.rem(step, 2)
        other = 1 - side
        await_all(recv_p.at[side, g], pr_sem.at[side, g])

        def expand(r, c):
            terms = recv_p[side, g, :, r].astype(F32).reshape(ntl * K, lanes)
            terms = jnp.transpose(terms)
            turned = swapped(terms, -1.0).astype(BF16)
            terms = terms.astype(BF16)
            ordered = None
            for half in range(PAIR):
                f = g * PAIR + half
                mine = dot(terms, base[other, f, r, 0]) + dot(turned, base[other, f, r, 1])
                ordered = mine if half == 0 else jnp.where(bin_row(NB) == half, mine, ordered)

            @pl.when(step > 0)
            def _():
                await_all(send_t.at[g, r, pl.ds(0, nfreq - 1)], ts_sem.at[g, r])

            send_t[g, r] = ordered.reshape(nfreq, inner, NB).astype(BF16)

            @pl.when((g > 0) | (r < tiles - 1))
            def _():
                results_out(g, r)

            @pl.when((g == 1) & (r == tiles - 2))
            def _():
                results_out(0, tiles - 1)

            return c

        lax.fori_loop(0, tiles, expand, 0)

    def time_work(step):
        side = lax.rem(step, 2)
        last = 2 * ITERS - 1

        def samples(r, c):
            for g in range(pairs):
                await_all(recv_t.at[r, g], tr_sem.at[r, g])
            arrived = recv_t[r].astype(F32).reshape(pairs * nfreq * inner, NB).astype(BF16)
            moments = lax.broadcasted_iota(jnp.int32, (nt, NB), 0)
            field = jnp.where(
                moments < onsets_ref[:, tile_cols(r)], dot(inv_ref[...], arrived), 0.0
            )

            @pl.when(step < last)
            def _():
                await_all(send_f.at[:, r, pl.ds(0, nfreq - 1)], fs_sem.at[r])
                values = field.astype(BF16)
                band(0, r, values)
                spectra_out(0, r)
                for g in range(1, pairs):
                    band(g, r, values)

            @pl.when((step < last) & (r == tiles - 2))
            def _():
                spectra_out(1, 0)

            fields[side, :, tile_cols(r)] += field
            return c

        lax.fori_loop(0, tiles, samples, 0)

        @pl.when(step < last)
        def _():
            def one(r, c):
                spectra_out(1, r)
                return c

            lax.fori_loop(1, tiles, one, 0)

    def half_step(step, carry):
        def one(i, c):
            order = jnp.where(i == 2, 3, jnp.where(i == 3, 2, i))
            coefficients(step, order // tiles, lax.rem(order, tiles))
            return c

        def two(g, c):
            expansion(step, g)
            return c

        lax.fori_loop(0, pairs * tiles, one, 0)
        lax.fori_loop(0, pairs, two, 0)
        time_work(step)
        return carry

    lax.fori_loop(0, 2 * ITERS, half_step, 0)

    def drain(r, c):
        await_all(send_f.at[:, r, pl.ds(0, nfreq - 1)], fs_sem.at[r])
        for g in range(pairs):
            await_all(send_t.at[g, r, pl.ds(0, nfreq - 1)], ts_sem.at[g, r])
            await_all(send_p.at[g, 0, pl.ds(0, ntl - tiles)], ps_sem.at[g, r])
        return c

    lax.fori_loop(0, tiles, drain, 0)
    await_all(right_raw.at[:, :, pl.ds(0, npts - 1)], base_send)


def body(ny, nz, npts, direct, onsets, left_bases, right_bases, tile_ranks):
    nfreq = ny * nz
    fh, tiles, ntl = left_bases.shape[:3]
    _, nt, cells = direct.shape
    pairs = fh // PAIR
    inner = 2 * PAIR
    forward, inverse = band_tables(fh * nfreq, nt, nfreq)
    tables = [jnp.asarray(t, dtype=BF16) for t in (forward, inverse)]
    hbm = pl.BlockSpec(memory_space=pl.ANY)
    dma = pltpu.SemaphoreType.DMA

    def in_hbm(array):
        return pltpu.with_memory_space_constraint(array, pltpu.HBM)

    fields = pl.pallas_call(
        functools.partial(kernel, ny, nz, npts),
        out_shape=jax.ShapeDtypeStruct((2, nt, cells), F32),
        in_specs=[hbm] * 7,
        out_specs=pl.BlockSpec(memory_space=pltpu.VMEM),
        scratch_shapes=[
            pltpu.VMEM((nt, cells), BF16),
            pltpu.VMEM((1, cells), jnp.int32),
            pltpu.SMEM((tiles, fh, ntl), jnp.int32),
            *[pltpu.VMEM(t.shape, BF16) for t in tables],
            pltpu.VMEM((2, fh, tiles, 2, ntl * K, NB), BF16),
            pltpu.VMEM((fh, tiles, ntl, 2, K, NB), BF16),
            pltpu.VMEM((pairs, tiles, npts, PAIR, tiles, 1, 2, K, NB), BF16),
            pltpu.VMEM((pairs, tiles, nfreq, inner, NB), BF16),
            pltpu.VMEM((pairs, tiles, nfreq, inner, NB), BF16),
            pltpu.VMEM((pairs, tiles, nfreq, inner, NB), BF16),
            pltpu.VMEM((tiles, pairs, nfreq, inner, NB), BF16),
            pltpu.VMEM((pairs, tiles, ntl, K, inner * nfreq), BF16),
            pltpu.VMEM((2, pairs, ntl, tiles, K, inner * nfreq), BF16),
            dma((6,)),
            dma,
            dma((pairs, tiles)),
            dma((tiles,)),
            dma((pairs, tiles)),
            dma((pairs, tiles)),
            dma((tiles, pairs)),
            dma((pairs, tiles)),
            dma((2, pairs)),
        ],
        compiler_params=pltpu.CompilerParams(
            collective_id=0, has_side_effects=True, vmem_limit_bytes=32 * 1024 * 1024
        ),
    )(
        in_hbm(direct),
        in_hbm(onsets),
        in_hbm(left_bases),
        in_hbm(right_bases),
        in_hbm(jnp.transpose(tile_ranks, (1, 0, 2))),
        *[in_hbm(t) for t in tables],
    )
    return fields[1:], fields[:1]


def solution(mesh):
    nfreq, npts = mesh.shape["freq"], mesh.shape["pts"]
    nz = NZ if nfreq > NZ else 4
    return jax.shard_map(
        functools.partial(body, nfreq // nz, nz, npts),
        mesh=mesh,
        in_specs=(
            P("freq", None, "pts"),
            P("freq", "pts"),
            P("freq", "pts", None, None, None, None),
            P("freq", "pts", None, None, None, None),
            P("freq", "pts", None),
        ),
        out_specs=(P("freq", None, "pts"), P("freq", None, "pts")),
        check_vma=False,
    )
```
